32 devices in a mesh: lat: 16 (over z, y, core), lon: 2 (over x).
Axes of the slice: x: 2, y: 2, z: 4, core: 2. Of those that a mesh axis runs over, the one named last changes fastest.
Arguments:
- eastward_speed_face: float32 [72, 512, 256], P(None, 'lat', 'lon'), may hold values from -6 to 6
- northward_speed_face: float32 [72, 512, 256], P(None, 'lat', 'lon'), may hold values from -6 to 6
- stratum_extent_east_face: float32 [72, 512, 256], P(None, 'lat', 'lon'), may hold values from 0.5 to 2
- stratum_extent_north_face: float32 [72, 512, 256], P(None, 'lat', 'lon'), may hold values from 0.5 to 2
- northward_span_east_face: float32 [512, 256], P('lat', 'lon'), may hold values from 0.5 to 2
- eastward_span_north_face: float32 [512, 256], P('lat', 'lon'), may hold values from 0.5 to 2
- ocean_flag_east_face: int32 [72, 512, 256], P(None, 'lat', 'lon'), may hold values 0 or 1
- ocean_flag_north_face: int32 [72, 512, 256], P(None, 'lat', 'lon'), may hold values 0 or 1
- counterpart_across_seam: int32 [256], replicated, may hold values from 0 to 255, as said below
Outputs:
- eastward_speed_next: float32 [72, 512, 256], P(None, 'lat', 'lon')
- northward_speed_next: float32 [72, 512, 256], P(None, 'lat', 'lon')
The draws below stay inside these ranges and needn't reach their ends.
Inputs may be any that keep to these rules, and one draw needn't show every extreme that they name: counterpart_across_seam[i] = (p - 1 - i) mod 256 for one pivot p drawn anew in each draw; it is its own inverse.
All inputs are finite; a program needn't handle non-finite values. No bound on the sum of `ocean_flag_east_face` or of `ocean_flag_north_face` on one device may be relied on, other than what follows from the above.
Results may differ from the reference program's by a relative error of at most 0.00002.
Values sent between devices are 32-bit elements; how exact they have to be, the bound alone decides.
A program may use at most 128 MiB of HBM per device.

```python
import math
import jax
import jax.numpy as jnp
from jax import lax

STRATA_COUNT = 72
NORTHWARD_CELLS = 512
EASTWARD_CELLS = 256


def draw_counterpart_across_seam(key, part):
    pivot = jax.random.randint(jax.random.fold_in(key, 17), (), 0, EASTWARD_CELLS)
    columns = jnp.arange(EASTWARD_CELLS, dtype=jnp.int32)
    return ((pivot - 1 - columns) % EASTWARD_CELLS).astype(jnp.int32)


def touch_ends(values, rng, low, high):
    longest = values.shape.index(max(values.shape))
    spots = []
    for shift in (0, 1):
        where = [jax.random.randint(jax.random.fold_in(rng, axis), (), 0, length) for axis, length in enumerate(values.shape)]
        where[longest] = (where[longest] + shift) % values.shape[longest]
        spots.append(tuple(where))
    return values.at[spots[0]].set(low).at[spots[1]].set(high)


def shard_levels(rng, shape, pieces, least, top_value):
    def one(dim, parts):
        draws = jax.random.uniform(jax.random.fold_in(jax.random.fold_in(rng, 6), dim), (parts,), jnp.float32, least / len(pieces), top_value / len(pieces))
        return jnp.repeat(jnp.exp(draws), shape[dim] // parts).reshape((-1,) + (1,) * (len(shape) - dim - 1))

    loudness = one(*pieces[0])
    for cut in pieces[1:]:
        loudness = loudness * one(*cut)
    return loudness


def centred(key, shape, scale, most, pieces=(), kind=jnp.bfloat16):
    loudness = shard_levels(key, shape, pieces, -0.22, 0.18) if pieces else 1.0
    values = jax.random.normal(key, shape, jnp.float32) * scale * loudness
    return jnp.minimum(jnp.maximum(values, -most), most).astype(kind)


def setup_inputs(seed: int = 0) -> dict:
    key_of = jax.random.split(jax.random.key(seed), 10)
    return {
        "eastward_speed_face": centred(key_of[0], (STRATA_COUNT, NORTHWARD_CELLS, EASTWARD_CELLS), 1.0, 6.0, ((1, 16), (2, 2)), jnp.float32),
        "northward_speed_face": centred(key_of[1], (STRATA_COUNT, NORTHWARD_CELLS, EASTWARD_CELLS), 1.0, 6.0, ((1, 16), (2, 2)), jnp.float32),
        "stratum_extent_east_face": jnp.clip(jnp.exp(math.log(2.0) - 1.3862944 * jax.random.uniform(key_of[2], (STRATA_COUNT, NORTHWARD_CELLS, EASTWARD_CELLS), jnp.float32) ** shard_levels(key_of[2], (STRATA_COUNT, NORTHWARD_CELLS, EASTWARD_CELLS), ((1, 16), (2, 2)), -0.2, 0.2)), 0.5, 2.0),
        "stratum_extent_north_face": jnp.clip(jnp.exp(math.log(2.0) - 1.3862944 * jax.random.uniform(key_of[3], (STRATA_COUNT, NORTHWARD_CELLS, EASTWARD_CELLS), jnp.float32) ** shard_levels(key_of[3], (STRATA_COUNT, NORTHWARD_CELLS, EASTWARD_CELLS), ((1, 16), (2, 2)), -0.2, 0.2)), 0.5, 2.0),
        "northward_span_east_face": jnp.clip(jnp.exp(math.log(2.0) - 1.3862944 * jax.random.uniform(key_of[4], (NORTHWARD_CELLS, EASTWARD_CELLS), jnp.float32) ** shard_levels(key_of[4], (NORTHWARD_CELLS, EASTWARD_CELLS), ((0, 16), (1, 2)), -0.2, 0.2)), 0.5, 2.0),
        "eastward_span_north_face": jnp.clip(jnp.exp(math.log(2.0) - 1.3862944 * jax.random.uniform(key_of[5], (NORTHWARD_CELLS, EASTWARD_CELLS), jnp.float32) ** shard_levels(key_of[5], (NORTHWARD_CELLS, EASTWARD_CELLS), ((0, 16), (1, 2)), -0.2, 0.2)), 0.5, 2.0),
        "ocean_flag_east_face": touch_ends((jax.random.randint(key_of[6], (STRATA_COUNT, NORTHWARD_CELLS, EASTWARD_CELLS), 0, 4) < 3).astype(jnp.int32), jax.random.fold_in(key_of[6], 1), 0, 1),
        "ocean_flag_north_face": touch_ends((jax.random.randint(key_of[7], (STRATA_COUNT, NORTHWARD_CELLS, EASTWARD_CELLS), 0, 4) < 3).astype(jnp.int32), jax.random.fold_in(key_of[7], 1), 0, 1),
        "counterpart_across_seam": draw_counterpart_across_seam(jax.random.fold_in(key_of[9], 71), 0),
    }


time_step = 0.2


def interp(a, b, c, d):
    return (7.0 * (b + c) - (a + d)) / 12.0


def advect(umv, vmv, tuv, tvv, rows, cols):
    def cx(field, ro, co):
        return field[..., ro:ro + rows, co:co + cols + 1]

    def ry(field, ro, co):
        return field[..., ro:ro + rows + 1, co:co + cols]

    fut = 0.5 * (cx(tuv, 2, 1) + cx(tuv, 2, 2)) * interp(cx(umv, 2, 0), cx(umv, 2, 1), cx(umv, 2, 2), cx(umv, 2, 3))
    vface = ry(tvv, 1, 2)
    fvf = 0.5 * (vface + ry(tvv, 1, 3)) * interp(ry(umv, 0, 2), ry(umv, 1, 2), ry(umv, 2, 2), ry(umv, 3, 2))
    fuf = 0.5 * (cx(tuv, 2, 1) + cx(tuv, 3, 1)) * interp(cx(vmv, 2, 0), cx(vmv, 2, 1), cx(vmv, 2, 2), cx(vmv, 2, 3))
    fvt = 0.5 * (vface + ry(tvv, 2, 2)) * interp(ry(vmv, 0, 2), ry(vmv, 1, 2), ry(vmv, 2, 2), ry(vmv, 3, 2))
    trend_u = -((fut[..., 1:] - fut[..., :-1]) + (fvf[..., 1:, :] - fvf[..., :-1, :]))
    trend_v = -((fuf[..., 1:] - fuf[..., :-1]) + (fvt[..., 1:, :] - fvt[..., :-1, :]))
    return trend_u, trend_v


def extend(field, counterpart_across_seam):
    north = -field[-2:, :][::-1, :][:, counterpart_across_seam]
    south = jnp.zeros((2, field.shape[1]), jnp.float32)
    padded = jnp.concatenate([south, field, north], axis=0)
    return jnp.concatenate([padded[:, -2:], padded, padded[:, :2]], axis=1)


def reference(eastward_speed_face, northward_speed_face, stratum_extent_east_face, stratum_extent_north_face, northward_span_east_face, eastward_span_north_face, ocean_flag_east_face, ocean_flag_north_face, counterpart_across_seam):
    def stratum_index(items):
        uk, vk, e3uk, e3vk, umk, vmk = items
        um = umk.astype(jnp.float32) * uk
        vm = vmk.astype(jnp.float32) * vk
        volu = northward_span_east_face * e3uk
        volv = eastward_span_north_face * e3vk
        tu = volu * um
        tv = volv * vm
        ext = [extend(f, counterpart_across_seam) for f in (um, vm, tu, tv)]
        trend_u, trend_v = advect(ext[0], ext[1], ext[2], ext[3], um.shape[0], um.shape[1])
        u_new = umk.astype(jnp.float32) * (um + time_step * trend_u / volu)
        v_new = vmk.astype(jnp.float32) * (vm + time_step * trend_v / volv)
        return u_new, v_new

    eastward_speed_next, northward_speed_next = lax.map(stratum_index, (eastward_speed_face, northward_speed_face, stratum_extent_east_face, stratum_extent_north_face, ocean_flag_east_face, ocean_flag_north_face))
    return eastward_speed_next, northward_speed_next
```

```python
import functools

import jax
import jax.numpy as jnp
from jax import lax
from jax.experimental import pallas as pl
from jax.experimental.pallas import tpu as pltpu
from jax.sharding import PartitionSpec as P

time_step = 0.2
lanes = 128
group = 8
spare = 8
MESH = pl.DeviceIdType.MESH


def chunk_count(levels):
    groups = levels // group
    return next(c for c in (3, 2, 1) if groups % c == 0)


def roll(x, shift):
    return pltpu.roll(x, shift % lanes, 1)


def exchange_kernel(
    nlat, nlon, levels, rows,
    u_hbm, v_hbm, eu_hbm, ev_hbm, su_hbm, sv_hbm, mu_hbm, mv_hbm,
    um_x, vm_x, tu_x, tv_x, cu_x, cv_x, packs, corner_u, corner_v, band,
    u_in, v_in, eu_in, ev_in, su_in, sv_in, mu_in, mv_in,
    pack_own, corner_u_own, corner_v_own,
    load_sem, span_sem, up_send, up_recv, down_send, down_recv,
    lon_send, lon_recv, diag_send, diag_recv, band_send, band_recv,
):
    chunks = chunk_count(levels)
    depth = levels // chunks
    lat = lax.axis_index("lat")
    lon = lax.axis_index("lon")
    right = lax.rem(lon + 1, nlon)
    left = lax.rem(lon + nlon - 1, nlon)
    has_up = lat < nlat - 1
    has_down = lat > 0
    sides = 1 if nlon == 2 else 2

    pairs = (
        (u_hbm, u_in), (mu_hbm, mu_in), (eu_hbm, eu_in),
        (v_hbm, v_in), (mv_hbm, mv_in), (ev_hbm, ev_in),
    )
    spans = [
        pltpu.make_async_copy(su_hbm, su_in, span_sem.at[0]),
        pltpu.make_async_copy(sv_hbm, sv_in, span_sem.at[1]),
    ]
    loads = [
        [
            pltpu.make_async_copy(
                a.at[pl.ds(c * depth, depth)], b.at[pl.ds(c * depth, depth), pl.ds(0, rows)], load_sem.at[c, k]
            )
            for k, (a, b) in enumerate(pairs)
        ]
        for c in range(chunks)
    ]
    for copy in spans:
        copy.start()
    for per_chunk in loads:
        for copy in per_chunk:
            copy.start()

    barrier = pltpu.get_barrier_semaphore()

    def greet(where):
        pl.semaphore_signal(barrier, inc=1, device_id=where, device_id_type=MESH)

    greet((lat, right))
    if nlon > 2:
        greet((lat, left))

    @pl.when(has_up)
    def _():
        greet((lat + 1, lon))
        greet((lat + 1, left))

    @pl.when(has_down)
    def _():
        greet((lat - 1, lon))
        greet((lat - 1, right))

    if nlon > 3:
        @pl.when(lat == nlat - 1)
        def _():
            for d in range(2, nlon - 1):
                greet((lat, lax.rem(lon + d, nlon)))

    def arrive():
        @pl.when(lat == 0)
        def _():
            pl.semaphore_wait(barrier, sides + 2)

        @pl.when(has_up & has_down)
        def _():
            pl.semaphore_wait(barrier, sides + 4)

        @pl.when(lat == nlat - 1)
        def _():
            pl.semaphore_wait(barrier, sides + 2 + max(nlon - 3, 0))

    def remote(src, dst, send, recv, where):
        return pltpu.make_async_remote_copy(
            src_ref=src, dst_ref=dst, send_sem=send, recv_sem=recv,
            device_id=where, device_id_type=MESH,
        )

    def up_copies(c):
        part = pl.ds(c * depth, depth)
        where = (lat + 1, lon)
        moves = (
            (um_x.at[pl.ds(rows, 2), part], um_x.at[pl.ds(0, 2), part]),
            (vm_x.at[pl.ds(rows, 2), part], vm_x.at[pl.ds(0, 2), part]),
            (tv_x.at[pl.ds(rows, 1), part], tv_x.at[pl.ds(0, 1), part]),
        )
        return [
            remote(a, b, up_send.at[c, k], up_recv.at[c, k], where)
            for k, (a, b) in enumerate(moves)
        ]

    def down_copies(c):
        part = pl.ds(c * depth, depth)
        where = (lat - 1, lon)
        moves = (
            (um_x.at[pl.ds(2, 2), part], um_x.at[pl.ds(rows + 2, 2), part]),
            (vm_x.at[pl.ds(2, 2), part], vm_x.at[pl.ds(rows + 2, 2), part]),
            (tu_x.at[pl.ds(0, 1), part], tu_x.at[pl.ds(rows, 1), part]),
            (tv_x.at[pl.ds(1, 1), part], tv_x.at[pl.ds(rows + 1, 1), part]),
        )
        return [
            remote(a, b, down_send.at[c, k], down_recv.at[c, k], where)
            for k, (a, b) in enumerate(moves)
        ]

    def lon_copies(c):
        part = pl.ds(c * depth, depth)
        targets = (right,) if nlon == 2 else (right, left)
        return [
            remote(
                pack_own.at[:, part], packs.at[k, :, part],
                lon_send.at[c, k], lon_recv.at[c, k], (lat, target),
            )
            for k, target in enumerate(targets)
        ]

    def corner_down():
        return remote(
            corner_u_own, corner_u, diag_send.at[0], diag_recv.at[0], (lat - 1, right)
        )

    def corner_up():
        return remote(
            corner_v_own, corner_v, diag_send.at[1], diag_recv.at[1], (lat + 1, left)
        )

    def band_copy(c, d):
        part = pl.ds(c * depth, depth)
        return remote(
            band.at[lon, :, part], band.at[lon, :, part],
            band_send.at[c, d], band_recv.at[c, d], (lat, lax.rem(lon + d, nlon)),
        )

    def band_arrival(c, d):
        part = pl.ds(c * depth, depth)
        origin = lax.rem(lon + nlon - d, nlon)
        return remote(
            band.at[lon, :, part], band.at[origin, :, part],
            band_send.at[c, d], band_recv.at[c, d], (lat, lax.rem(lon + d, nlon)),
        )

    lane = lax.broadcasted_iota(jnp.int32, (group, lanes), 1)
    quad = lane // 4
    place = lane % 4
    pitch = rows + spare
    views = [ref.reshape(levels * pitch, lanes) for _, ref in pairs]

    def compute(g, corners):
        cu_corner, cv_corner = corners
        base = g * group
        part = pl.ds(pl.multiple_of(base, group), group)
        zero = jnp.zeros((group, lanes), jnp.float32)
        pack_u, pack_v, pack_t = zero, zero, zero
        for r in range(rows):
            u, mu, eu, v, mv, ev = [
                view[pl.ds(base * pitch + r, group, stride=pitch), :] for view in views
            ]
            mu = mu.astype(jnp.float32)
            mv = mv.astype(jnp.float32)
            um = mu * u
            vm = mv * v
            vol_u = su_in[pl.ds(r, 1), :] * eu
            vol_v = sv_in[pl.ds(r, 1), :] * ev
            tu = vol_u * um
            tv = vol_v * vm
            um_x[r + 2, part, :] = um
            vm_x[r + 2, part, :] = vm
            tu_x[r, part, :] = tu
            tv_x[r + 1, part, :] = tv
            cu_x[r, part, :] = mu * (-time_step / 24.0) / vol_u
            cv_x[r, part, :] = mv * (-time_step / 24.0) / vol_v
            here = quad == r
            pack_u = jnp.where(here, roll(um, 2 + 4 * r), pack_u)
            pack_v = jnp.where(here, roll(vm, 2 + 4 * r), pack_v)
            both = jnp.where(place < 2, roll(tu, 1 + 4 * r), roll(tv, 3 + 4 * r))
            pack_t = jnp.where(here, both, pack_t)
            if r == 0:
                cu_corner = jnp.where(lane == g, pltpu.roll(tu, g + 1, 1), cu_corner)
            if r == rows - 1:
                cv_corner = jnp.where(lane == g, pltpu.roll(tv, g, 1), cv_corner)
                band[lon, 4, part, :] = tu
                band[lon, 5, part, :] = tv
            if r >= rows - 2:
                band[lon, r - rows + 2, part, :] = um
                band[lon, r - rows + 4, part, :] = vm
        pack_own[0, part, :] = pack_u
        pack_own[1, part, :] = pack_v
        pack_own[2, part, :] = pack_t
        return cu_corner, cv_corner

    @pl.when(lat == 0)
    def _():
        um_x[pl.ds(0, 2)] = jnp.zeros((2, levels, lanes), jnp.float32)
        vm_x[pl.ds(0, 2)] = jnp.zeros((2, levels, lanes), jnp.float32)
        tv_x[pl.ds(0, 1)] = jnp.zeros((1, levels, lanes), jnp.float32)
        corner_v[...] = jnp.zeros((group, lanes), jnp.float32)

    for copy in spans:
        copy.wait()
    corners = (jnp.zeros((group, lanes), jnp.float32),) * 2
    for c in range(chunks):
        for copy in loads[c]:
            copy.wait()
        per = depth // group
        corners = lax.fori_loop(c * per, (c + 1) * per, compute, corners)
        if c == 0:
            arrive()

        for copy in lon_copies(c):
            copy.start()

        @pl.when(has_down)
        def _():
            for copy in down_copies(c):
                copy.start()

        @pl.when(has_up)
        def _():
            for copy in up_copies(c):
                copy.start()

        @pl.when(lat == nlat - 1)
        def _():
            for d in range(1, nlon):
                band_copy(c, d).start()

    corner_u_own[...], corner_v_own[...] = corners

    @pl.when(has_down)
    def _():
        corner_down().start()

    @pl.when(has_up)
    def _():
        corner_up().start()

    for c in range(chunks):
        for copy in lon_copies(c):
            copy.wait()

        @pl.when(has_down)
        def _():
            for copy in down_copies(c):
                copy.wait_send()
            for copy in up_copies(c):
                copy.wait_recv()

        @pl.when(has_up)
        def _():
            for copy in up_copies(c):
                copy.wait_send()
            for copy in down_copies(c):
                copy.wait_recv()

        @pl.when(lat == nlat - 1)
        def _():
            for d in range(1, nlon):
                band_copy(c, d).wait_send()
                band_arrival(c, d).wait_recv()

    @pl.when(has_down)
    def _():
        corner_down().wait_send()
        corner_up().wait_recv()

    @pl.when(has_up)
    def _():
        corner_up().wait_send()
        corner_down().wait_recv()


def stencil_kernel(
    nlat, nlon, levels, rows,
    fold_ref, um_x, vm_x, tu_x, tv_x, cu_x, cv_x, packs, corner_u, corner_v, band,
    u_out, v_out,
    high, high_left, beside, moved, u_buf, v_buf, out_sem,
):
    lat = lax.axis_index("lat")
    lon = lax.axis_index("lon")
    groups = levels // group
    width = nlon * lanes
    lane = lax.broadcasted_iota(jnp.int32, (group, lanes), 1)
    top = lat == nlat - 1

    @pl.when(top)
    def _():
        first = fold_ref[0]
        own = lax.rem(first - lon * lanes - lane + 2 * width, width)
        before = jnp.zeros_like(lane) + lax.rem(first - lon * lanes + 1 + 2 * width, width)

        def pick(k, part, index):
            block = index // lanes
            spot = index % lanes
            got = jnp.zeros((group, lanes), jnp.float32)
            for b in range(nlon):
                taken = jnp.take_along_axis(
                    band[b, k, part, :], spot, axis=1, mode="promise_in_bounds"
                )
                got = jnp.where(block == b, taken, got)
            return -got

        def fill(g, carry):
            part = pl.ds(pl.multiple_of(g * group, group), group)
            high[0, part, :] = pick(1, part, own)
            high[1, part, :] = pick(0, part, own)
            high[2, part, :] = pick(3, part, own)
            high[3, part, :] = pick(2, part, own)
            high[4, part, :] = pick(4, part, own)
            high[5, part, :] = pick(5, part, own)
            high_left[part, :] = pick(4, part, before)
            return carry

        lax.fori_loop(0, groups, fill, 0)

    @pl.when(lat < nlat - 1)
    def _():
        def fill(g, carry):
            part = pl.ds(pl.multiple_of(g * group, group), group)
            high[0, part, :] = um_x[rows + 2, part, :]
            high[1, part, :] = um_x[rows + 3, part, :]
            high[2, part, :] = vm_x[rows + 2, part, :]
            high[3, part, :] = vm_x[rows + 3, part, :]
            high[4, part, :] = tu_x[rows, part, :]
            high[5, part, :] = tv_x[rows + 1, part, :]
            high_left[part, :] = pltpu.roll(corner_u[...], lanes - 1 - g, 1)
            return carry

        lax.fori_loop(0, groups, fill, 0)

    place = lane % 4
    pitch = rows + spare
    u_view = u_buf.reshape(levels * pitch, lanes)
    v_view = v_buf.reshape(levels * pitch, lanes)

    def q(a, b, c, d):
        return 7.0 * (b + c) - (a + d)

    def out_copies(g):
        part = pl.ds(g * group, group)
        return (
            pltpu.make_async_copy(u_buf.at[part, pl.ds(0, rows)], u_out.at[part], out_sem.at[g, 0]),
            pltpu.make_async_copy(v_buf.at[part, pl.ds(0, rows)], v_out.at[part], out_sem.at[g, 1]),
        )

    def readers(part):
        def um(j):
            return um_x[j + 2, part, :] if j < rows else high[j - rows, part, :]

        def vm(j):
            return vm_x[j + 2, part, :] if j < rows else high[j - rows + 2, part, :]

        def tu(j):
            return tu_x[j, part, :] if j < rows else high[4, part, :]

        def tv(j):
            return tv_x[j + 1, part, :] if j < rows else high[5, part, :]

        return um, vm, tu, tv

    def unpack(g, carry):
        part = pl.ds(pl.multiple_of(g * group, group), group)
        if packs.shape[0] == 1:
            pack_u, pack_v, pack_t = [packs[0, k, part, :] for k in range(3)]
        else:
            pack_u, pack_v = [
                jnp.where(place < 2, packs[0, k, part, :], packs[1, k, part, :])
                for k in range(2)
            ]
            pack_t = jnp.where(place < 1, packs[0, 2, part, :], packs[1, 2, part, :])
        for j in range(rows):
            beside[0, j, part, :] = roll(pack_u, -(4 * j + 2))
            beside[1, j, part, :] = roll(pack_v, -(4 * j + 2))
            beside[2, j, part, :] = roll(pack_t, -(4 * j + 1))
            beside[3, j, part, :] = roll(pack_t, -(4 * j + 3))
        return carry

    lax.fori_loop(0, groups, unpack, 0)

    def shift(g, carry):
        part = pl.ds(pl.multiple_of(g * group, group), group)
        um, vm, tu, tv = readers(part)
        tv_low = jnp.where(
            lane == 0, pltpu.roll(corner_v[...], lax.rem(lanes - g, lanes), 1), tv(-1)
        )
        moved[11, 0, part, :] = roll(tv_low, -1)
        moved[11, 1, part, :] = roll(
            jnp.where(lane == lanes - 1, high_left[part, :], tu(rows)), 1
        )
        for j in range(rows):
            for k, own in ((0, um(j)), (4, vm(j))):
                halo = beside[k // 4, j, part, :]
                low = jnp.where(lane >= lanes - 2, halo, own)
                upper = jnp.where(lane < 2, halo, own)
                moved[k, j, part, :] = roll(low, 2)
                moved[k + 1, j, part, :] = roll(jnp.where(lane == lanes - 1, halo, own), 1)
                moved[k + 2, j, part, :] = roll(jnp.where(lane == 0, halo, own), -1)
                moved[k + 3, j, part, :] = roll(upper, -2)
            own, halo = tu(j), beside[2, j, part, :]
            moved[8, j, part, :] = roll(jnp.where(lane == lanes - 1, halo, own), 1)
            moved[9, j, part, :] = roll(jnp.where(lane == 0, halo, own), -1)
            moved[10, j, part, :] = roll(jnp.where(lane == 0, beside[3, j, part, :], tv(j)), -1)
        return carry

    lax.fori_loop(0, groups, shift, 0)

    def step(g, carry):
        part = pl.ds(pl.multiple_of(g * group, group), group)
        um, vm, tu, tv = readers(part)

        def tu_sides(j):
            if j < rows:
                return tu(j), moved[8, j, part, :], moved[9, j, part, :]
            return tu(j), moved[11, 1, part, :], None

        def around(k, j, own):
            w2, w1, e1, e2 = [moved[k + i, j, part, :] for i in range(4)]
            return q(w2, w1, own, e1), q(w1, own, e1, e2)

        def fvf(j):
            east = moved[11, 0, part, :] if j < 0 else moved[10, j, part, :]
            return (tv(j) + east) * q(um(j - 1), um(j), um(j + 1), um(j + 2))

        def fvt(j):
            return (tv(j - 1) + tv(j)) * q(vm(j - 2), vm(j - 1), vm(j), vm(j + 1))

        fvf_low = fvf(-1)
        fvt_low = fvt(0)
        tu_own, tu_west, tu_east = tu_sides(0)
        for j in range(rows):
            fvf_high = fvf(j)
            fvt_high = fvt(j + 1)
            um_own = um(j)
            vm_own = vm(j)
            q_west, q_east = around(0, j, um_own)
            du = (tu_own + tu_east) * q_east - (tu_west + tu_own) * q_west
            du = du + (fvf_high - fvf_low)
            next_own, next_west, next_east = tu_sides(j + 1)
            q_west, q_east = around(4, j, vm_own)
            dv = (tu_own + next_own) * q_east - (tu_west + next_west) * q_west
            dv = dv + (fvt_high - fvt_low)
            where = pl.ds(g * (group * pitch) + j, group, stride=pitch)
            u_view[where, :] = um_own + cu_x[j, part, :] * du
            v_view[where, :] = vm_own + cv_x[j, part, :] * dv
            fvf_low, fvt_low = fvf_high, fvt_high
            tu_own, tu_west, tu_east = next_own, next_west, next_east
        for copy in out_copies(g):
            copy.start()
        return carry

    lax.fori_loop(0, groups, step, 0)

    def finish(g, carry):
        for copy in out_copies(g):
            copy.wait()
        return carry

    lax.fori_loop(0, groups, finish, 0)


def local(nlat, nlon, u, v, eu, ev, su, sv, mu, mv, fold):
    u, v, eu, ev, su, sv, mu, mv = [
        pltpu.with_memory_space_constraint(x, pltpu.HBM) for x in (u, v, eu, ev, su, sv, mu, mv)
    ]
    levels, rows, _ = u.shape
    chunks = chunk_count(levels)
    sides = 1 if nlon == 2 else 2
    f32 = jnp.float32
    vmem = pl.BlockSpec(memory_space=pltpu.VMEM)
    hbm = pl.BlockSpec(memory_space=pltpu.HBM)
    shapes = [
        (rows + 4, levels, lanes),
        (rows + 4, levels, lanes),
        (rows + 1, levels, lanes),
        (rows + 2, levels, lanes),
        (rows, levels, lanes),
        (rows, levels, lanes),
        (sides, 3, levels, lanes),
        (group, lanes),
        (group, lanes),
        (nlon, 6, levels, lanes),
    ]
    block = (levels, rows, lanes)
    roomy = (levels, rows + spare, lanes)
    dma = pltpu.SemaphoreType.DMA
    fields = pl.pallas_call(
        functools.partial(exchange_kernel, nlat, nlon, levels, rows),
        out_shape=[pltpu.VMEM(s, f32) for s in shapes],
        in_specs=[hbm] * 8,
        out_specs=[vmem] * len(shapes),
        scratch_shapes=[
            pltpu.VMEM(roomy, f32),
            pltpu.VMEM(roomy, f32),
            pltpu.VMEM(roomy, f32),
            pltpu.VMEM(roomy, f32),
            pltpu.VMEM((rows, lanes), f32),
            pltpu.VMEM((rows, lanes), f32),
            pltpu.VMEM(roomy, jnp.int32),
            pltpu.VMEM(roomy, jnp.int32),
            pltpu.VMEM((3, levels, lanes), f32),
            pltpu.VMEM((group, lanes), f32),
            pltpu.VMEM((group, lanes), f32),
            dma((chunks, 6)),
            dma((2,)),
            dma((chunks, 3)),
            dma((chunks, 3)),
            dma((chunks, 4)),
            dma((chunks, 4)),
            dma((chunks, sides)),
            dma((chunks, sides)),
            dma((2,)),
            dma((2,)),
            dma((chunks, nlon)),
            dma((chunks, nlon)),
        ],
        compiler_params=pltpu.CompilerParams(
            collective_id=0, has_side_effects=True, vmem_limit_bytes=16 * 1024 * 1024
        ),
        name="exchange",
    )(u, v, eu, ev, su, sv, mu, mv)
    result = pl.pallas_call(
        functools.partial(stencil_kernel, nlat, nlon, levels, rows),
        out_shape=[jax.ShapeDtypeStruct(block, f32)] * 2,
        in_specs=[pl.BlockSpec(memory_space=pltpu.SMEM)] + [vmem] * len(shapes),
        out_specs=[hbm] * 2,
        scratch_shapes=[
            pltpu.VMEM((6, levels, lanes), f32),
            pltpu.VMEM((levels, lanes), f32),
            pltpu.VMEM((4, rows, levels, lanes), f32),
            pltpu.VMEM((12, rows, levels, lanes), f32),
            pltpu.VMEM(roomy, f32),
            pltpu.VMEM(roomy, f32),
            dma((levels // group, 2)),
        ],
        compiler_params=pltpu.CompilerParams(vmem_limit_bytes=32 * 1024 * 1024),
        name="stencil",
    )(fold, *fields)
    return tuple(result)


def solution(mesh):
    level_rows_columns = P(None, "lat", "lon")
    return jax.shard_map(
        functools.partial(local, mesh.shape["lat"], mesh.shape["lon"]),
        mesh=mesh,
        in_specs=(
            level_rows_columns,
            level_rows_columns,
            level_rows_columns,
            level_rows_columns,
            P("lat", "lon"),
            P("lat", "lon"),
            level_rows_columns,
            level_rows_columns,
            P(),
        ),
        out_specs=(level_rows_columns,) * 2,
        check_vma=False,
    )
```
